256 devices in a mesh: replica: 8 (over x_lo, y), expert: 16 (over z, core), tensor: 2 (over x_hi).
Axes of the slice: x: 4 (x_hi: 2, x_lo: 2; x = x_hi * 2 + x_lo), y: 4, z: 8, core: 2. Of those that a mesh axis runs over, the one named last changes fastest.
Arguments:
- delta: bfloat16 [8, 256, 16, 14336], P('replica', 'expert', None, 'tensor'), may hold values from -6 to 6
- step_offsets: int32 [8], replicated, may hold values from 0 to 15, as said below
- block_map: int32 [256], replicated, may hold values from 0 to 255, as said below
- master_params: float32 [256, 16, 14336], P('expert', 'replica', 'tensor'), may hold values from -6 to 6
- first_moment: float32 [256, 16, 14336], P('expert', 'replica', 'tensor'), may hold values from -2 to 2
- second_moment: float32 [256, 16, 14336], P('expert', 'replica', 'tensor'), may hold values from 0.01 to 1
Outputs:
- new_params: bfloat16 [256, 16, 14336], P('expert', 'replica')
- new_first: float32 [256, 16, 14336], P('expert', 'replica', 'tensor')
- new_second: float32 [256, 16, 14336], P('expert', 'replica', 'tensor')
The draws below stay inside these ranges and needn't reach their ends.
Inputs may be any that keep to these rules, and one draw needn't show every extreme that they name: `block_map`: A permutation of the block indices onto owner slots; slot s belongs to expert index s // 16, and the blocks b with b // 16 = i go in equal numbers to every expert index. `step_offsets`: the replica groups' offsets are distinct.
All inputs are finite; a program needn't handle non-finite values.
Results may differ from the reference program's by a relative error of at most 0.0035.
Values may be sent and summed in bfloat16 or wider, within the bound.
A program may use at most 64 MiB of HBM per device.

```python
import math
import jax
import jax.numpy as jnp
from jax import lax

FF = 14336
BLK_DEV = 16
BR = 16
BLOCKS = 256
REPLICAS = 8


def shuffled(key_one):
    return jax.random.permutation(key_one, BLK_DEV)


def draw_block_map(key, part):
    owners = BLOCKS // BLK_DEV
    first_key = jax.random.fold_in(key, 11)
    second_key = jax.random.fold_in(key, 23)
    source_perm = jax.vmap(shuffled)(jax.random.split(first_key, owners)).astype(jnp.int32)
    target = source_perm % owners
    ordinal = source_perm // owners
    sources = jnp.arange(owners, dtype=jnp.int32)[:, None]
    arrival = sources * (BLK_DEV // owners) + ordinal
    owner_perm = jax.vmap(shuffled)(jax.random.split(second_key, owners)).astype(jnp.int32)
    slot_ids = owner_perm[target, arrival]
    return (target * BLK_DEV + slot_ids).reshape(BLOCKS).astype(jnp.int32)


def draw_step_offsets(key, part):
    inner_key = jax.random.fold_in(key, 37)
    order_key = jax.random.fold_in(key, 41)
    middle = jax.random.permutation(inner_key, jnp.arange(1, 15, dtype=jnp.int32))[:REPLICAS - 2]
    ends = jnp.array([0, 15], dtype=jnp.int32)
    values = jnp.concatenate([ends, middle.astype(jnp.int32)])
    return jax.random.permutation(order_key, values).astype(jnp.int32)


def spiked(drawn, stream_key, source, target, blocks, factor):
    owner, partner = [(jnp.arange(drawn.shape[position]) // (drawn.shape[position] // blocks)).reshape([-1 if axis == position else 1 for axis in range(drawn.ndim)]) for position in (source, target)]
    chosen = jax.random.permutation(stream_key, blocks)[partner]
    strong = (owner == chosen) | (owner == (partner + blocks // 2) % blocks)
    return jnp.where(strong, factor * drawn, drawn)


def shard_levels(own_key, shape, shards, low, high):
    factor_of = 1.0
    for axis_at, parts in shards:
        heights = jax.random.uniform(jax.random.fold_in(jax.random.fold_in(own_key, 6), axis_at), (parts,), jnp.float32, low / len(shards), high / len(shards))
        factor_of = factor_of * jnp.repeat(jnp.exp(heights), shape[axis_at] // parts).reshape((-1,) + (1,) * (len(shape) - 1 - axis_at))
    return factor_of


def noise(own_key, dims, scale, most, pieces=(), held_as=jnp.bfloat16):
    level = shard_levels(own_key, dims, pieces, -0.22, 0.18) if pieces else 1.0
    drawn = jax.random.normal(own_key, dims, jnp.float32) * scale * level
    return jnp.minimum(jnp.maximum(drawn, -most), most).astype(held_as)


def bell_draw_with(own_key, extent, width, limit, shards, heavy, held_as=jnp.bfloat16):
    values = width * jax.random.normal(own_key, extent, jnp.float32)
    if shards:
        values = values * shard_levels(own_key, extent, shards, -0.22, 0.18)
    return jnp.clip(spiked(values, jax.random.fold_in(own_key, 3), *heavy), -limit, limit).astype(held_as)


def setup_inputs(seed: int = 0) -> dict:
    key_list = jax.random.split(jax.random.key(seed), 7)
    return {
        "delta": bell_draw_with(key_list[0], (REPLICAS, BLOCKS, BR, FF), 1.0, 6.0, ((0, 8), (1, 16), (3, 2)), (0, 2, 8, 2.0)),
        "step_offsets": draw_step_offsets(jax.random.fold_in(key_list[6], 71), 0),
        "block_map": draw_block_map(jax.random.fold_in(key_list[6], 71), 0),
        "master_params": noise(key_list[3], (BLOCKS, BR, FF), 1.0, 6.0, ((0, 16), (1, 8), (2, 2)), jnp.float32),
        "first_moment": noise(key_list[4], (BLOCKS, BR, FF), 0.3, 2.0, ((0, 16), (1, 8), (2, 2)), jnp.float32),
        "second_moment": jnp.clip(jnp.exp(math.log(1.0) - 4.6051702 * jax.random.uniform(key_list[5], (BLOCKS, BR, FF), jnp.float32) ** shard_levels(key_list[5], (BLOCKS, BR, FF), ((0, 16), (1, 8), (2, 2)), -0.2, 0.2)), 0.01, 1.0),
    }


beta_one = 0.9
beta_two = 0.99
outer_rate = 0.7
outer_round = 20
epsilon = 1e-08

def replica_weights(step_offsets):
    reciprocal = 1.0 / (1.0 + step_offsets.astype(jnp.float32))
    return reciprocal / jnp.sum(reciprocal)

def adam_update(gradient, master_params, first_moment, second_moment):
    new_first = beta_one * first_moment + (1.0 - beta_one) * gradient
    new_second = beta_two * second_moment + (1.0 - beta_two) * gradient * gradient
    fix_one = 1.0 - beta_one ** outer_round
    fix_two = 1.0 - beta_two ** outer_round
    update_step = new_first / fix_one / (jnp.sqrt(new_second / fix_two) + epsilon)
    new_params = (master_params - outer_rate * update_step).astype(jnp.bfloat16)
    return (new_params, new_first, new_second)

def reference(delta, step_offsets, block_map, master_params, first_moment, second_moment):
    weights = replica_weights(step_offsets)

    def add_replica(replica_id, running):
        slice_rows = lax.dynamic_index_in_dim(delta, replica_id, 0, keepdims=False).astype(jnp.float32)
        scaled = (slice_rows * weights[replica_id]).astype(jnp.bfloat16)
        scaled = lax.optimization_barrier(scaled)
        return running + scaled.astype(jnp.float32)
    pseudo = lax.fori_loop(0, REPLICAS, add_replica, jnp.zeros(delta.shape[1:], jnp.float32))
    inverse = jnp.argsort(block_map).astype(jnp.int32)
    gradient = pseudo[inverse]
    new_params, new_first, new_second = adam_update(gradient, master_params, first_moment, second_moment)
    return (new_params, new_first, new_second)
```

```python
import functools

import jax
import jax.numpy as jnp
from jax import lax
from jax.experimental import pallas as pl
from jax.experimental.pallas import tpu as pltpu
from jax.sharding import PartitionSpec as P

beta_one = 0.9
beta_two = 0.99
outer_rate = 0.7
outer_round = 20
epsilon = 1e-08

MESH = pl.DeviceIdType.MESH
F32 = jnp.float32
BF16 = jnp.bfloat16

CHUNKS = (1, 1, 1, 1, 1, 1, 1)
LANES = 128
TILES = 8
RING = 4
UNROLL = 4


def adam(gradient, master, first, second):
    new_first = beta_one * first + (1.0 - beta_one) * gradient
    new_second = beta_two * second + (1.0 - beta_two) * gradient * gradient
    fix_one = 1.0 - beta_one**outer_round
    fix_two = 1.0 - beta_two**outer_round
    step = new_first / fix_one / (jnp.sqrt(new_second / fix_two) + epsilon)
    return (master - outer_rate * step).astype(BF16), new_first, new_second


def kernel(experts, blocks, refs):
    chunks = len(CHUNKS)
    starts = [sum(CHUNKS[:k]) for k in range(chunks)]
    (offsets_ref, map_ref, delta_ref, master_ref, first_ref, second_ref) = refs[:6]
    (params_out, first_out, second_out) = refs[6:9]
    scratch = list(refs[9:])

    def take(n):
        got = scratch[:n]
        del scratch[:n]
        return got

    delta_v = take(chunks)
    weighted = take(chunks)
    far = take(chunks)
    passed = take(chunks)
    plain = take(chunks)
    xsend = take(chunks)
    xrecv = take(chunks)
    zsend = take(chunks)
    zrecv = take(chunks)
    master_v = take(chunks)
    first_v = take(chunks)
    second_v = take(chunks)
    params_v = take(chunks)
    (spread, woven) = take(2)
    (order_s, source_s) = take(2)
    (in_sem, out_sem, far_send, far_recv, pass_send, pass_recv, plain_send, plain_recv) = take(8)
    (x_send, x_recv, z_send, z_recv, t_send, t_recv) = take(6)

    replica = lax.axis_index("replica")
    expert = lax.axis_index("expert")
    tensor = lax.axis_index("tensor")
    x = replica // RING
    y = replica % RING
    up = (y + 1) % RING
    down = (y + RING - 1) % RING
    across = (y + 2) % RING
    device_up = {"replica": x * RING + up}
    device_down = {"replica": x * RING + down}
    device_x = {"replica": (1 - x) * RING + y}
    device_t = {"tensor": 1 - tensor}

    barrier = pltpu.get_barrier_semaphore()
    for device in (device_up, device_down, device_x, device_t):
        pl.semaphore_signal(barrier, inc=1, device_id=device, device_id_type=MESH)

    def greet(d, carry):
        pl.semaphore_signal(
            barrier, inc=1, device_id={"expert": (expert + d) % experts}, device_id_type=MESH
        )
        return carry

    lax.fori_loop(1, experts, greet, 0)

    def load_delta(k):
        rows = pl.ds(starts[k] * TILES * 8, CHUNKS[k] * TILES * 8)
        return pltpu.make_async_copy(delta_ref.at[:, :, rows, :], delta_v[k], in_sem.at[k])

    def load_states(k):
        rows = pl.ds(starts[k] * 16, CHUNKS[k] * 16)
        return [
            pltpu.make_async_copy(ref.at[:, rows, :], held[k], in_sem.at[(n + 1) * chunks + k])
            for n, (ref, held) in enumerate(
                ((master_ref, master_v), (first_ref, first_v), (second_ref, second_v))
            )
        ]

    for k in range(chunks):
        load_delta(k).start()
    for k in range(chunks):
        for copy in load_states(k):
            copy.start()

    def find_order(b, held):
        target = lax.shift_right_logical(map_ref[expert * blocks + b], 4)
        return tuple(jnp.where(target == j, b, held[j]) for j in range(experts))

    order = lax.fori_loop(0, blocks, find_order, (jnp.int32(0),) * experts)
    for j in range(experts):
        order_s[j] = order[j]

    def find_source(i, held):
        slot = jnp.int32(0)
        for b in range(blocks):
            offset = map_ref[i * blocks + b] - expert * blocks
            slot = jnp.where((offset >= 0) & (offset < blocks), offset, slot)
        return tuple(jnp.where(slot == s, i, held[s]) for s in range(blocks))

    source = lax.fori_loop(0, experts, find_source, (jnp.int32(0),) * blocks)
    for s in range(blocks):
        source_s[s] = source[s]

    reciprocal = 1.0 / (1.0 + offsets_ref[...].astype(F32))
    weights = reciprocal / jnp.sum(reciprocal, axis=1, keepdims=True)
    lane = lax.broadcasted_iota(jnp.int32, weights.shape, 1)
    weight = jnp.sum(jnp.where(lane == replica, weights, 0.0), axis=1, keepdims=True)

    def remote(src, dst, send, recv, device):
        return pltpu.make_async_remote_copy(
            src_ref=src, dst_ref=dst, send_sem=send, recv_sem=recv, device_id=device, device_id_type=MESH
        )

    def far_copies(k):
        return [
            remote(weighted[k].at[across], far[k].at[0], far_send.at[2 * k], far_recv.at[2 * k], device_up),
            remote(
                weighted[k].at[RING + across], far[k].at[1], far_send.at[2 * k + 1], far_recv.at[2 * k + 1], device_down
            ),
        ]

    def pass_copies(k):
        return [
            remote(far[k].at[0], passed[k].at[0], pass_send.at[2 * k], pass_recv.at[2 * k], device_up),
            remote(far[k].at[1], passed[k].at[1], pass_send.at[2 * k + 1], pass_recv.at[2 * k + 1], device_down),
        ]

    def plain_copies(k):
        return [
            remote(
                weighted[k].at[RING + up], plain[k].at[1], plain_send.at[2 * k], plain_recv.at[2 * k], device_up
            ),
            remote(
                weighted[k].at[down], plain[k].at[0], plain_send.at[2 * k + 1], plain_recv.at[2 * k + 1], device_down
            ),
        ]

    def x_copy(k):
        return remote(xsend[k], xrecv[k], x_send.at[k], x_recv.at[k], device_x)

    def z_copy(k, j):
        return remote(zsend[k].at[j], zrecv[k].at[expert], z_send.at[k], z_recv.at[k], {"expert": j})

    def own_rows(k):
        whole = CHUNKS[k] * 16
        return pl.ds(pl.multiple_of(tensor * (sum(CHUNKS) * 16) + starts[k] * 16, 16), whole)

    def t_copy(k):
        return remote(params_v[k], params_out.at[:, own_rows(k), :], t_send.at[k], t_recv.at[k], device_t)

    def stores(k):
        rows = pl.ds(starts[k] * 16, CHUNKS[k] * 16)
        return [
            pltpu.make_async_copy(params_v[k], params_out.at[:, own_rows(k), :], out_sem.at[k]),
            pltpu.make_async_copy(first_v[k], first_out.at[:, rows, :], out_sem.at[chunks + k]),
            pltpu.make_async_copy(second_v[k], second_out.at[:, rows, :], out_sem.at[2 * chunks + k]),
        ]

    def weigh(k):
        units = CHUNKS[k]
        load_delta(k).wait()

        def some(g, carry):
            for n in range(UNROLL):
                j = g * UNROLL + n
                for h in range(2):
                    spread[n, h, : units * 64, :] = delta_v[k][order_s[j], h].astype(F32) * weight
                for h in range(2):
                    for q in range(RING):
                        for unit in range(units):
                            pair = [
                                spread[n, h, pl.ds(unit * 64 + 2 * q + row, TILES, stride=8), :] for row in range(2)
                            ]
                            weighted[k][RING * h + q, j, unit * 16 : unit * 16 + 16, :] = jnp.concatenate(
                                pair, axis=0
                            ).astype(BF16)
            return carry

        lax.fori_loop(0, experts // UNROLL, some, 0)

    def loop(step):
        def some(g, carry):
            for n in range(UNROLL):
                step(g * UNROLL + n)
            return carry

        lax.fori_loop(0, experts // UNROLL, some, 0)

    def add_on_way(k):
        for copy in far_copies(k):
            copy.wait_recv()

        def step(j):
            for n, place in ((0, up), (1, RING + down)):
                total = far[k][n, j].astype(F32) + weighted[k][place, j].astype(F32)
                far[k][n, j] = total.astype(BF16)

        loop(step)

    def ring_sum(k, h, j):
        total = weighted[k][RING * h + y, j].astype(F32) + plain[k][h, j].astype(F32)
        return total + passed[k][h, j].astype(F32)

    def x_half(k):
        for copy in pass_copies(k) + plain_copies(k):
            copy.wait_recv()

        def step(j):
            xsend[k][j] = ring_sum(k, 1 - x, j).astype(BF16)

        loop(step)
        x_copy(k).start()

    def finish(k):
        x_copy(k).wait_recv()

        def step(j):
            zsend[k][j] = (ring_sum(k, x, j) + xrecv[k][j].astype(F32)).astype(BF16)

        loop(step)

        def send(d, carry):
            z_copy(k, (expert + d) % experts).start()
            return carry

        lax.fori_loop(1, experts, send, 0)
        zrecv[k][expert] = zsend[k][expert]

    def all_of(k, ref, sem):
        return pltpu.make_async_copy(ref.at[: experts - 1], ref.at[: experts - 1], sem.at[k])

    def update(k):
        all_of(k, zrecv[k], z_recv).wait()
        for copy in load_states(k):
            copy.wait()

        def step(s, n):
            arrived = zrecv[k][source_s[s]].astype(F32)
            for unit in range(CHUNKS[k]):
                for row in range(2):
                    woven[n, pl.ds(unit * 16 + row, TILES, stride=2), :] = arrived[
                        unit * 16 + row * 8 : unit * 16 + row * 8 + 8
                    ]
            rows = CHUNKS[k] * 16
            params_v[k][s], first_v[k][s], second_v[k][s] = adam(
                woven[n, :rows], master_v[k][s], first_v[k][s], second_v[k][s]
            )

        def some(g, carry):
            for n in range(UNROLL):
                step(g * UNROLL + n, n)
            return carry

        lax.fori_loop(0, blocks // UNROLL, some, 0)
        t_copy(k).start()
        for copy in stores(k):
            copy.start()

    for t in range(chunks + 4):
        if t < chunks:
            weigh(t)
            if t == 0:
                pl.semaphore_wait(barrier, experts + 3)
            for copy in far_copies(t):
                copy.start()
        if 0 <= t - 1 < chunks:
            add_on_way(t - 1)
            for copy in pass_copies(t - 1):
                copy.start()
        if t < chunks:
            for copy in plain_copies(t):
                copy.start()
        if 0 <= t - 2 < chunks:
            x_half(t - 2)
        if 0 <= t - 3 < chunks:
            finish(t - 3)
        if 0 <= t - 4 < chunks:
            update(t - 4)

    for k in range(chunks):
        for copy in far_copies(k) + pass_copies(k) + plain_copies(k) + [x_copy(k)]:
            copy.wait_send()
        all_of(k, zsend[k], z_send).wait()
        t_copy(k).wait()
        for copy in stores(k):
            copy.wait()


def fused(experts, blocks, *operands):
    chunks = len(CHUNKS)
    units = sum(CHUNKS)
    wide = max(CHUNKS)

    def each(*lead, dtype=BF16):
        return [pltpu.VMEM((*lead, n * 16, LANES), dtype) for n in CHUNKS]

    scratch = [pltpu.VMEM((blocks, 2, n * 64, LANES), BF16) for n in CHUNKS]
    scratch += each(2 * RING, experts)
    scratch += each(2, experts) + each(2, experts) + each(2, experts)
    scratch += each(experts) + each(experts) + each(experts) + each(experts)
    scratch += each(blocks, dtype=F32) + each(blocks, dtype=F32) + each(blocks, dtype=F32) + each(blocks)
    scratch += [pltpu.VMEM((UNROLL, 2, wide * 64, LANES), F32), pltpu.VMEM((UNROLL, wide * 16, LANES), F32)]
    scratch += [pltpu.SMEM((experts,), jnp.int32), pltpu.SMEM((blocks,), jnp.int32)]
    scratch += [pltpu.SemaphoreType.DMA((n * chunks,)) for n in (4, 3, 2, 2, 2, 2, 2, 2, 1, 1, 1, 1, 1, 1)]
    anywhere = pl.BlockSpec(memory_space=pl.ANY)
    return pl.pallas_call(
        lambda *refs: kernel(experts, blocks, refs),
        name="outer_step",
        out_shape=(
            jax.ShapeDtypeStruct((blocks, 2 * units * 16, LANES), BF16),
            jax.ShapeDtypeStruct((blocks, units * 16, LANES), F32),
            jax.ShapeDtypeStruct((blocks, units * 16, LANES), F32),
        ),
        in_specs=[
            pl.BlockSpec(memory_space=pltpu.VMEM),
            pl.BlockSpec(memory_space=pltpu.SMEM),
            anywhere,
            anywhere,
            anywhere,
            anywhere,
        ],
        out_specs=(anywhere, anywhere, anywhere),
        scratch_shapes=scratch,
        compiler_params=pltpu.CompilerParams(
            collective_id=0, has_side_effects=True, vmem_limit_bytes=60 * 1024 * 1024
        ),
    )(*operands)


def tiled(value, rows):
    lead = value.shape[:-2]
    tall, columns = value.shape[-2:]
    split = value.reshape(*lead, tall // rows, rows, columns // LANES, LANES)
    return jnp.swapaxes(split, -3, -2).reshape(*lead, tall // rows, columns // LANES * rows, LANES)


def untiled(value):
    lead, tall, lanes = value.shape
    split = value.reshape(lead, tall // 2, 2, lanes)
    return jnp.swapaxes(split, 1, 2).reshape(lead, 2, tall // 2 * lanes)


def body(experts, delta, step_offsets, block_map, master_params, first_moment, second_moment):
    blocks = master_params.shape[0]
    states = [tiled(value, 2)[:, 0] for value in (master_params, first_moment, second_moment)]
    outs = fused(experts, blocks, step_offsets[None], block_map, tiled(delta[0], 8), *states)
    return tuple(untiled(value) for value in outs)


def solution(mesh):
    in_specs = (
        P("replica", "expert", None, "tensor"),
        P(),
        P(),
        P("expert", "replica", "tensor"),
        P("expert", "replica", "tensor"),
        P("expert", "replica", "tensor"),
    )
    out_specs = (
        P("expert", "replica", None),
        P("expert", "replica", "tensor"),
        P("expert", "replica", "tensor"),
    )
    step = functools.partial(body, mesh.shape["expert"])
    return jax.shard_map(step, mesh=mesh, in_specs=in_specs, out_specs=out_specs, check_vma=False)
```

```python
import functools

import jax
import jax.numpy as jnp
from jax import lax
from jax.experimental import pallas as pl
from jax.experimental.pallas import tpu as pltpu
from jax.sharding import PartitionSpec as P

beta_one = 0.9
beta_two = 0.99
outer_rate = 0.7
outer_round = 20
epsilon = 1e-08

MESH = pl.DeviceIdType.MESH
F32 = jnp.float32
BF16 = jnp.bfloat16

CHUNKS = (1, 1, 1, 1, 1, 1, 1)
FIRST = "yyyyxxx"
ORDER = (
    "W4", "W0", "W1", "L0", "W5", "L1", "P0", "P1", "D4", "L4", "W6", "W2", "X0", "W3", "X1", "P4", "L2", "D5", "P2", "P3", "Z4", "L3", "P5", "D6", "X2", "Z0", "L5", "U4", "L6", "Z1", "X3", "Z2", "P6", "Z5", "U0", "Z3", "Z6", "U1", "U2", "U5", "U3", "U6",
)
LANES = 128
TILES = 8
RING = 4
UNROLL = 4


def adam(gradient, master, first, second):
    new_first = beta_one * first + (1.0 - beta_one) * gradient
    new_second = beta_two * second + (1.0 - beta_two) * gradient * gradient
    fix_one = 1.0 - beta_one**outer_round
    fix_two = 1.0 - beta_two**outer_round
    step = new_first / fix_one / (jnp.sqrt(new_second / fix_two) + epsilon)
    return (master - outer_rate * step).astype(BF16), new_first, new_second


def kernel(experts, blocks, refs):
    chunks = len(CHUNKS)
    starts = [sum(CHUNKS[:k]) for k in range(chunks)]
    (offsets_hbm, map_hbm, delta_ref, master_ref, first_ref, second_ref) = refs[:6]
    (params_out, first_out, second_out) = refs[6:9]
    scratch = list(refs[9:])

    def take(n):
        got = scratch[:n]
        del scratch[:n]
        return got

    delta_v = take(chunks)
    weighted = take(chunks)
    far = take(chunks)
    passed = take(chunks)
    plain = take(chunks)
    xsend = take(chunks)
    xrecv = take(chunks)
    zsend = take(chunks)
    zrecv = take(chunks)
    master_v = take(chunks)
    first_v = take(chunks)
    second_v = take(chunks)
    (spread, woven) = take(2)
    (offsets_ref, map_ref, order_s, source_s) = take(4)
    (small_sem, in_sem, far_send, far_recv, pass_send, pass_recv, plain_send, plain_recv) = take(8)
    (x_send, x_recv, z_send, z_recv, t_send, t_recv) = take(6)

    replica = lax.axis_index("replica")
    expert = lax.axis_index("expert")
    tensor = lax.axis_index("tensor")
    x = replica // RING
    y = replica % RING
    up = (y + 1) % RING
    down = (y + RING - 1) % RING
    across = (y + 2) % RING
    device_up = {"replica": x * RING + up}
    device_down = {"replica": x * RING + down}
    device_x = {"replica": (1 - x) * RING + y}
    device_t = {"tensor": 1 - tensor}

    barrier = pltpu.get_barrier_semaphore()
    for device in (device_up, device_down, device_x, device_t):
        pl.semaphore_signal(barrier, inc=1, device_id=device, device_id_type=MESH)

    def greet(d, carry):
        pl.semaphore_signal(
            barrier, inc=1, device_id={"expert": (expert + d) % experts}, device_id_type=MESH
        )
        return carry

    lax.fori_loop(1, experts, greet, 0)

    def load_delta(k):
        rows = pl.ds(starts[k] * TILES * 8, CHUNKS[k] * TILES * 8)
        return pltpu.make_async_copy(delta_ref.at[:, :, rows, :], delta_v[k], in_sem.at[k])

    def load_states(k):
        rows = pl.ds(starts[k] * 16, CHUNKS[k] * 16)
        return [
            pltpu.make_async_copy(ref.at[:, rows, :], held[k], in_sem.at[(n + 1) * chunks + k])
            for n, (ref, held) in enumerate(
                ((master_ref, master_v), (first_ref, first_v), (second_ref, second_v))
            )
        ]

    load_map = pltpu.make_async_copy(map_hbm, map_ref, small_sem.at[0])
    load_offsets = pltpu.make_async_copy(offsets_hbm, offsets_ref, small_sem.at[1])
    load_map.start()
    load_offsets.start()
    for k in range(chunks):
        load_delta(k).start()
    for k in range(chunks):
        for copy in load_states(k):
            copy.start()

    load_map.wait()

    def find_order(b, held):
        target = lax.shift_right_logical(map_ref[expert * blocks + b], 4)
        return tuple(jnp.where(target == j, b, held[j]) for j in range(experts))

    order = lax.fori_loop(0, blocks, find_order, (jnp.int32(0),) * experts)
    for j in range(experts):
        order_s[j] = order[j]

    load_offsets.wait()
    reciprocal = 1.0 / (1.0 + offsets_ref[...].astype(F32))
    weights = reciprocal / jnp.sum(reciprocal, axis=1, keepdims=True)
    lane = lax.broadcasted_iota(jnp.int32, weights.shape, 1)
    weight = jnp.sum(jnp.where(lane == replica, weights, 0.0), axis=1, keepdims=True)

    def find_sources():
        def find_source(i, held):
            slot = jnp.int32(0)
            for b in range(blocks):
                offset = map_ref[i * blocks + b] - expert * blocks
                slot = jnp.where((offset >= 0) & (offset < blocks), offset, slot)
            return tuple(jnp.where(slot == s, i, held[s]) for s in range(blocks))

        source = lax.fori_loop(0, experts, find_source, (jnp.int32(0),) * blocks)
        for s in range(blocks):
            source_s[s] = source[s]

    def remote(src, dst, send, recv, device):
        return pltpu.make_async_remote_copy(
            src_ref=src, dst_ref=dst, send_sem=send, recv_sem=recv, device_id=device, device_id_type=MESH
        )

    half = experts // 2
    low, high = pl.ds(0, half), pl.ds(half, half)

    def both_ways(k, up_from, up_to, down_from, down_to, send, recv):
        return [
            remote(up_from, up_to, send.at[2 * k], recv.at[2 * k], device_up),
            remote(down_from, down_to, send.at[2 * k + 1], recv.at[2 * k + 1], device_down),
        ]

    def far_copies(k):
        if FIRST[k] == "y":
            ends = (weighted[k].at[across], far[k].at[0], weighted[k].at[RING + across], far[k].at[1])
        else:
            ends = (xsend[k].at[across, low], far[k].at[low], xsend[k].at[across, high], far[k].at[high])
        return both_ways(k, *ends, far_send, far_recv)

    def pass_copies(k):
        if FIRST[k] == "y":
            ends = (far[k].at[0], passed[k].at[0], far[k].at[1], passed[k].at[1])
        else:
            ends = (far[k].at[low], passed[k].at[low], far[k].at[high], passed[k].at[high])
        return both_ways(k, *ends, pass_send, pass_recv)

    def plain_copies(k):
        if FIRST[k] == "y":
            ends = (weighted[k].at[RING + up], plain[k].at[1], weighted[k].at[down], plain[k].at[0])
        else:
            ends = (xsend[k].at[up, high], plain[k].at[high], xsend[k].at[down, low], plain[k].at[low])
        return both_ways(k, *ends, plain_send, plain_recv)

    def x_copy(k):
        source = xsend[k] if FIRST[k] == "y" else weighted[k].at[pl.ds(RING * (1 - x), RING)]
        return remote(source, xrecv[k], x_send.at[k], x_recv.at[k], device_x)

    def z_copy(k, j):
        return remote(zsend[k].at[j], zrecv[k].at[expert], z_send.at[k], z_recv.at[k], {"expert": j})

    def own_rows(k):
        whole = CHUNKS[k] * 16
        return pl.ds(pl.multiple_of(tensor * (sum(CHUNKS) * 16) + starts[k] * 16, 16), whole)

    def t_copy(k):
        return remote(params_out.at[:, own_rows(k), :], params_out.at[:, own_rows(k), :], t_send.at[k], t_recv.at[k], device_t)

    def weigh(k):
        units = CHUNKS[k]
        load_delta(k).wait()

        def some(g, carry):
            for n in range(UNROLL):
                j = g * UNROLL + n
                for h in range(2):
                    spread[n, h, : units * 64, :] = delta_v[k][order_s[j], h].astype(F32) * weight
                for h in range(2):
                    for q in range(RING):
                        for unit in range(units):
                            pair = [
                                spread[n, h, pl.ds(unit * 64 + 2 * q + row, TILES, stride=8), :] for row in range(2)
                            ]
                            weighted[k][RING * h + q, j, unit * 16 : unit * 16 + 16, :] = jnp.concatenate(
                                pair, axis=0
                            ).astype(BF16)
            return carry

        lax.fori_loop(0, experts // UNROLL, some, 0)

    def loop(step):
        def some(g, carry):
            for n in range(UNROLL):
                step(g * UNROLL + n)
            return carry

        lax.fori_loop(0, experts // UNROLL, some, 0)

    def add_x(k):
        x_copy(k).wait_recv()

        def step(j):
            for q in range(RING):
                total = weighted[k][RING * x + q, j].astype(F32) + xrecv[k][q, j].astype(F32)
                xsend[k][q, j] = total.astype(BF16)

        loop(step)

    def add_on_way(k):
        for copy in far_copies(k):
            copy.wait_recv()

        def step(j):
            for n, place in ((0, up), (1, RING + down)):
                total = far[k][n, j].astype(F32) + weighted[k][place, j].astype(F32)
                far[k][n, j] = total.astype(BF16)

        def step_half(g, carry):
            for n in range(2):
                for base, place in ((0, up), (half, down)):
                    j = base + g * 2 + n
                    far[k][j] = (far[k][j].astype(F32) + xsend[k][place, j].astype(F32)).astype(BF16)
            return carry

        if FIRST[k] == "y":
            loop(step)
        else:
            lax.fori_loop(0, half // 2, step_half, 0)

    def ring_sum(k, h, j):
        if FIRST[k] == "y":
            terms = (weighted[k].at[RING * h + y], plain[k].at[h], passed[k].at[h])
        else:
            terms = (xsend[k].at[y], plain[k], passed[k])
        return terms[0][j].astype(F32) + terms[1][j].astype(F32) + terms[2][j].astype(F32)

    def wait_ring(k):
        for copy in pass_copies(k) + plain_copies(k):
            copy.wait_recv()

    def x_half(k):
        wait_ring(k)

        def step(j):
            xsend[k][j] = ring_sum(k, 1 - x, j).astype(BF16)

        loop(step)

    def finish(k):
        if FIRST[k] == "y":
            x_copy(k).wait_recv()
        else:
            wait_ring(k)

        def step(j):
            total = ring_sum(k, x, j)
            if FIRST[k] == "y":
                total = total + xrecv[k][j].astype(F32)
            zsend[k][j] = total.astype(BF16)

        loop(step)

        def send(i, carry):
            turn = i // 2
            hops = (turn + 1) // 2 * (1 - 2 * (turn % 2))
            z = (expert // 2 + experts // 4 + hops + experts) % (experts // 2)
            z_copy(k, 2 * z + (expert + 1 + i) % 2).start()
            return carry

        lax.fori_loop(0, experts - 1, send, 0)
        zrecv[k][expert] = zsend[k][expert]

    def all_of(k, ref, sem):
        return pltpu.make_async_copy(ref.at[: experts - 1], ref.at[: experts - 1], sem.at[k])

    def update(k):
        all_of(k, zrecv[k], z_recv).wait()
        for copy in load_states(k):
            copy.wait()

        def step(s, n):
            arrived = zrecv[k][source_s[s]].astype(F32)
            for unit in range(CHUNKS[k]):
                for row in range(2):
                    woven[n, pl.ds(unit * 16 + row, TILES, stride=2), :] = arrived[
                        unit * 16 + row * 8 : unit * 16 + row * 8 + 8
                    ]
            rows = CHUNKS[k] * 16
            (params, first, second) = adam(woven[n, :rows], master_v[k][s], first_v[k][s], second_v[k][s])
            params_out[s, own_rows(k), :] = params
            first_out[s, pl.ds(starts[k] * 16, rows), :] = first
            second_out[s, pl.ds(starts[k] * 16, rows), :] = second

        def some(g, carry):
            for n in range(UNROLL):
                step(g * UNROLL + n, n)
            return carry

        lax.fori_loop(0, blocks // UNROLL, some, 0)

    for n, (stage, number) in enumerate(ORDER):
        k = int(number)
        copies = []
        if stage == "W":
            weigh(k)
            copies = far_copies(k) if FIRST[k] == "y" else [x_copy(k)]
        elif stage == "D":
            add_x(k)
            copies = far_copies(k)
        elif stage == "P":
            add_on_way(k)
            copies = pass_copies(k)
        elif stage == "L":
            copies = plain_copies(k)
        elif stage == "X" and FIRST[k] == "y":
            x_half(k)
            copies = [x_copy(k)]
        elif stage == "Z":
            finish(k)
        elif stage == "U":
            update(k)
            copies = [t_copy(k)]
        if n == 0:
            pl.semaphore_wait(barrier, experts + 3)
        for copy in copies:
            copy.start()
        if n == 0:
            find_sources()

    for k in range(chunks):
        for copy in far_copies(k) + pass_copies(k) + plain_copies(k) + [x_copy(k)]:
            copy.wait_send()
        all_of(k, zsend[k], z_send).wait()
        t_copy(k).wait()


def fused(experts, blocks, *operands):
    chunks = len(CHUNKS)
    units = sum(CHUNKS)
    wide = max(CHUNKS)

    def each(*lead, dtype=BF16):
        return [pltpu.VMEM((*lead, n * 16, LANES), dtype) for n in CHUNKS]

    scratch = [pltpu.VMEM((blocks, 2, n * 64, LANES), BF16) for n in CHUNKS]
    def by_order(first, then):
        return [
            pltpu.VMEM((*(first if way == "y" else then), n * 16, LANES), BF16) for n, way in zip(CHUNKS, FIRST)
        ]

    scratch += each(2 * RING, experts)
    for _ in range(3):
        scratch += by_order((2, experts), (experts,))
    for _ in range(2):
        scratch += by_order((experts,), (RING, experts))
    scratch += each(experts) + each(experts)
    scratch += each(blocks, dtype=F32) + each(blocks, dtype=F32) + each(blocks, dtype=F32)
    scratch += [pltpu.VMEM((UNROLL, 2, wide * 64, LANES), F32), pltpu.VMEM((UNROLL, wide * 16, LANES), F32)]
    scratch += [pltpu.VMEM(operands[0].shape, jnp.int32), pltpu.SMEM(operands[1].shape, jnp.int32)]
    scratch += [pltpu.SMEM((experts,), jnp.int32), pltpu.SMEM((blocks,), jnp.int32)]
    scratch += [pltpu.SemaphoreType.DMA((n,)) for n in (2,)]
    scratch += [pltpu.SemaphoreType.DMA((n * chunks,)) for n in (4, 2, 2, 2, 2, 2, 2, 1, 1, 1, 1, 1, 1)]
    return pl.pallas_call(
        lambda *refs: kernel(experts, blocks, refs),
        name="outer_step",
        out_shape=(
            pltpu.VMEM((blocks, 2 * units * 16, LANES), BF16),
            pltpu.VMEM((blocks, units * 16, LANES), F32),
            pltpu.VMEM((blocks, units * 16, LANES), F32),
        ),
        in_specs=[pl.BlockSpec(memory_space=pltpu.HBM)] * len(operands),
        out_specs=(pl.BlockSpec(memory_space=pltpu.VMEM),) * 3,
        scratch_shapes=scratch,
        compiler_params=pltpu.CompilerParams(
            collective_id=0, has_side_effects=True, vmem_limit_bytes=32 * 1024 * 1024
        ),
    )(*(pltpu.with_memory_space_constraint(value, pltpu.HBM) for value in operands))


def tiled(value, rows):
    lead = value.shape[:-2]
    tall, columns = value.shape[-2:]
    split = value.reshape(*lead, tall // rows, rows, columns // LANES, LANES)
    return jnp.swapaxes(split, -3, -2).reshape(*lead, tall // rows, columns // LANES * rows, LANES)


def untiled(value):
    lead, tall, lanes = value.shape
    split = value.reshape(lead, tall // 2, 2, lanes)
    return jnp.swapaxes(split, 1, 2).reshape(lead, 2, tall // 2 * lanes)


def body(experts, delta, step_offsets, block_map, master_params, first_moment, second_moment):
    blocks = master_params.shape[0]
    states = [tiled(value, 2)[:, 0] for value in (master_params, first_moment, second_moment)]
    outs = fused(experts, blocks, step_offsets[None], block_map, tiled(delta[0], 8), *states)
    return tuple(untiled(value) for value in outs)


def solution(mesh):
    in_specs = (
        P("replica", "expert", None, "tensor"),
        P(),
        P(),
        P("expert", "replica", "tensor"),
        P("expert", "replica", "tensor"),
        P("expert", "replica", "tensor"),
    )
    out_specs = (
        P("expert", "replica", None),
        P("expert", "replica", "tensor"),
        P("expert", "replica", "tensor"),
    )
    step = functools.partial(body, mesh.shape["expert"])
    return jax.shard_map(step, mesh=mesh, in_specs=in_specs, out_specs=out_specs, check_vma=False)
```

```python
import functools

import jax
import jax.numpy as jnp
from jax import lax
from jax.experimental import pallas as pl
from jax.experimental.pallas import tpu as pltpu
from jax.sharding import PartitionSpec as P

beta_one = 0.9
beta_two = 0.99
outer_rate = 0.7
outer_round = 20
epsilon = 1e-08

MESH = pl.DeviceIdType.MESH
F32 = jnp.float32
BF16 = jnp.bfloat16

CHUNKS = (1, 1, 1, 1, 1, 1, 1)
FIRST = "yyyyxxz"
ORDER = (
    "W6", "W3", "W2", "W0", "L2", "L0", "S0", "W4", "P2", "W1", "L3", "P0", "P3", "D6", "X2", "W5", "D4", "P1", "Z2", "L4", "P4", "L1", "X0", "E6", "X3", "Z4", "D5", "X1", "L5", "Z0", "L6", "P6", "Z3", "P5", "U2", "Z1", "U6", "U4", "Z5", "U0", "U3", "U1", "U5",
)
LANES = 128
TILES = 8
RING = 4
UNROLL = 4


def adam(gradient, master, first, second):
    new_first = beta_one * first + (1.0 - beta_one) * gradient
    new_second = beta_two * second + (1.0 - beta_two) * gradient * gradient
    fix_one = 1.0 - beta_one**outer_round
    fix_two = 1.0 - beta_two**outer_round
    step = new_first / fix_one / (jnp.sqrt(new_second / fix_two) + epsilon)
    return (master - outer_rate * step).astype(BF16), new_first, new_second


def kernel(experts, blocks, refs):
    chunks = len(CHUNKS)
    starts = [sum(CHUNKS[:k]) for k in range(chunks)]
    (offsets_hbm, map_hbm, delta_ref, master_ref, first_ref, second_ref) = refs[:6]
    (params_out, first_out, second_out) = refs[6:9]
    scratch = list(refs[9:])

    def take(n):
        got = scratch[:n]
        del scratch[:n]
        return got

    delta_v = take(chunks)
    weighted = take(chunks)
    far = take(chunks)
    passed = take(chunks)
    plain = take(chunks)
    xsend = take(chunks)
    xrecv = take(chunks)
    zsend = take(chunks)
    zrecv = take(chunks)
    master_v = take(chunks)
    first_v = take(chunks)
    second_v = take(chunks)
    (spread, woven) = take(2)
    (offsets_ref, map_ref, order_s, source_s) = take(4)
    (small_sem, in_sem, far_send, far_recv, pass_send, pass_recv, plain_send, plain_recv) = take(8)
    (x_send, x_recv, z_send, z_recv, t_send, t_recv) = take(6)

    replica = lax.axis_index("replica")
    expert = lax.axis_index("expert")
    tensor = lax.axis_index("tensor")
    x = replica // RING
    y = replica % RING
    up = (y + 1) % RING
    down = (y + RING - 1) % RING
    across = (y + 2) % RING
    device_up = {"replica": x * RING + up}
    device_down = {"replica": x * RING + down}
    device_x = {"replica": (1 - x) * RING + y}
    device_t = {"tensor": 1 - tensor}

    barrier = pltpu.get_barrier_semaphore()
    for device in (device_up, device_down, device_x, device_t):
        pl.semaphore_signal(barrier, inc=1, device_id=device, device_id_type=MESH)

    def greet(d, carry):
        pl.semaphore_signal(
            barrier, inc=1, device_id={"expert": (expert + d) % experts}, device_id_type=MESH
        )
        return carry

    lax.fori_loop(1, experts, greet, 0)

    def load_delta(k):
        rows = pl.ds(starts[k] * TILES * 8, CHUNKS[k] * TILES * 8)
        return pltpu.make_async_copy(delta_ref.at[:, :, rows, :], delta_v[k], in_sem.at[k])

    def load_states(k):
        rows = pl.ds(starts[k] * 16, CHUNKS[k] * 16)
        return [
            pltpu.make_async_copy(ref.at[:, rows, :], held[k], in_sem.at[(n + 1) * chunks + k])
            for n, (ref, held) in enumerate(
                ((master_ref, master_v), (first_ref, first_v), (second_ref, second_v))
            )
        ]

    load_map = pltpu.make_async_copy(map_hbm, map_ref, small_sem.at[0])
    load_offsets = pltpu.make_async_copy(offsets_hbm, offsets_ref, small_sem.at[1])
    load_map.start()
    load_offsets.start()
    for k in range(chunks):
        load_delta(k).start()
    for k in range(chunks):
        for copy in load_states(k):
            copy.start()

    load_offsets.wait()
    reciprocal = 1.0 / (1.0 + offsets_ref[...].astype(F32))
    weights = reciprocal / jnp.sum(reciprocal, axis=1, keepdims=True)
    lane = lax.broadcasted_iota(jnp.int32, weights.shape, 1)
    weight = jnp.sum(jnp.where(lane == replica, weights, 0.0), axis=1, keepdims=True)

    def look_up():
        load_map.wait()

        def find_order(b, held):
            target = lax.shift_right_logical(map_ref[expert * blocks + b], 4)
            return tuple(jnp.where(target == j, b, held[j]) for j in range(experts))

        order = lax.fori_loop(0, blocks, find_order, (jnp.int32(0),) * experts)
        for j in range(experts):
            order_s[j] = order[j]

        def find_source(i, held):
            slot = jnp.int32(0)
            for b in range(blocks):
                owner = map_ref[i * blocks + b]
                slot = jnp.where(lax.shift_right_logical(owner, 4) == expert, owner, slot)
            slot = slot - expert * blocks
            return tuple(jnp.where(slot == s, i, held[s]) for s in range(blocks))

        source = lax.fori_loop(0, experts, find_source, (jnp.int32(0),) * blocks)
        for s in range(blocks):
            source_s[s] = source[s]

    def remote(src, dst, send, recv, device):
        return pltpu.make_async_remote_copy(
            src_ref=src, dst_ref=dst, send_sem=send, recv_sem=recv, device_id=device, device_id_type=MESH
        )

    half = experts // 2
    low, high = pl.ds(0, half), pl.ds(half, half)

    def both_ways(k, up_from, up_to, down_from, down_to, send, recv):
        return [
            remote(up_from, up_to, send.at[2 * k], recv.at[2 * k], device_up),
            remote(down_from, down_to, send.at[2 * k + 1], recv.at[2 * k + 1], device_down),
        ]

    def y_term(k, place, rows):
        return xsend[k].at[place, rows] if FIRST[k] == "x" else zrecv[k].at[rows, place]

    def far_copies(k):
        if FIRST[k] == "y":
            ends = (weighted[k].at[across], far[k].at[0], weighted[k].at[RING + across], far[k].at[1])
        else:
            ends = (y_term(k, across, low), far[k].at[low], y_term(k, across, high), far[k].at[high])
        return both_ways(k, *ends, far_send, far_recv)

    def pass_copies(k):
        if FIRST[k] == "y":
            ends = (far[k].at[0], passed[k].at[0], far[k].at[1], passed[k].at[1])
        else:
            ends = (far[k].at[low], passed[k].at[low], far[k].at[high], passed[k].at[high])
        return both_ways(k, *ends, pass_send, pass_recv)

    def plain_copies(k):
        if FIRST[k] == "y":
            ends = (weighted[k].at[RING + up], plain[k].at[1], weighted[k].at[down], plain[k].at[0])
        else:
            ends = (y_term(k, up, high), plain[k].at[high], y_term(k, down, low), plain[k].at[low])
        return both_ways(k, *ends, plain_send, plain_recv)

    def x_copy(k):
        source = xsend[k] if FIRST[k] == "y" else weighted[k].at[pl.ds(RING * (1 - x), RING)]
        return remote(source, xrecv[k], x_send.at[k], x_recv.at[k], device_x)

    def z_copy(k, j):
        return remote(zsend[k].at[j], zrecv[k].at[expert], z_send.at[k], z_recv.at[k], {"expert": j})

    def own_rows(k):
        whole = CHUNKS[k] * 16
        return pl.ds(pl.multiple_of(tensor * (sum(CHUNKS) * 16) + starts[k] * 16, 16), whole)

    def t_copy(k):
        return remote(params_out.at[:, own_rows(k), :], params_out.at[:, own_rows(k), :], t_send.at[k], t_recv.at[k], device_t)

    def weigh(k):
        units = CHUNKS[k]
        load_delta(k).wait()

        def some(g, carry):
            for n in range(UNROLL):
                j = g * UNROLL + n
                for h in range(2):
                    spread[n, h, : units * 64, :] = delta_v[k][j, h].astype(F32) * weight
                for h in range(2):
                    for q in range(RING):
                        for unit in range(units):
                            pair = [
                                spread[n, h, pl.ds(unit * 64 + 2 * q + row, TILES, stride=8), :] for row in range(2)
                            ]
                            weighted[k][RING * h + q, j, unit * 16 : unit * 16 + 16, :] = jnp.concatenate(
                                pair, axis=0
                            ).astype(BF16)
            return carry

        lax.fori_loop(0, experts // UNROLL, some, 0)

    def loop(step):
        def some(g, carry):
            for n in range(UNROLL):
                step(g * UNROLL + n)
            return carry

        lax.fori_loop(0, experts // UNROLL, some, 0)

    def add_x(k):
        x_copy(k).wait_recv()

        def x_sum(q, j):
            return (weighted[k][RING * x + q, j].astype(F32) + xrecv[k][q, j].astype(F32)).astype(BF16)

        def step(j):
            for q in range(RING):
                if FIRST[k] == "x":
                    xsend[k][q, j] = x_sum(q, j)
                else:
                    zsend[k][j, q] = x_sum(q, order_s[j])

        loop(step)

    def add_on_way(k):
        for copy in far_copies(k):
            copy.wait_recv()

        def step(j):
            for n, place in ((0, up), (1, RING + down)):
                total = far[k][n, j].astype(F32) + weighted[k][place, j].astype(F32)
                far[k][n, j] = total.astype(BF16)

        def step_half(g, carry):
            for n in range(2):
                for base, place in ((0, up), (half, down)):
                    j = base + g * 2 + n
                    own = xsend[k][place, j] if FIRST[k] == "x" else zrecv[k][j, place]
                    far[k][j] = (far[k][j].astype(F32) + own.astype(F32)).astype(BF16)
            return carry

        if FIRST[k] == "y":
            loop(step)
        else:
            lax.fori_loop(0, half // 2, step_half, 0)

    def ring_sum(k, h, j):
        if FIRST[k] == "y":
            terms = (weighted[k][RING * h + y, j], plain[k][h, j], passed[k][h, j])
        elif FIRST[k] == "x":
            terms = (xsend[k][y, j], plain[k][j], passed[k][j])
        else:
            terms = (zrecv[k][j, y], plain[k][j], passed[k][j])
        return terms[0].astype(F32) + terms[1].astype(F32) + terms[2].astype(F32)

    def wait_ring(k):
        for copy in pass_copies(k) + plain_copies(k):
            copy.wait_recv()

    def x_half(k):
        wait_ring(k)

        def step(j):
            xsend[k][j] = ring_sum(k, 1 - x, j).astype(BF16)

        loop(step)

    def finish(k):
        if FIRST[k] == "y":
            x_copy(k).wait_recv()
        else:
            wait_ring(k)

        def step(j):
            block = order_s[j]
            total = ring_sum(k, x, block)
            if FIRST[k] == "y":
                total = total + xrecv[k][block].astype(F32)
            zsend[k][j] = total.astype(BF16)

        loop(step)

    def to_owners(k):
        def send(i, carry):
            turn = i // 2
            hops = (turn + 1) // 2 * (1 - 2 * (turn % 2))
            z = (expert // 2 + experts // 4 + hops + experts) % (experts // 2)
            z_copy(k, 2 * z + (expert + 1 + i) % 2).start()
            return carry

        lax.fori_loop(0, experts - 1, send, 0)
        zrecv[k][expert] = zsend[k][expert]

    def all_of(k, ref, sem):
        return pltpu.make_async_copy(ref.at[: experts - 1], ref.at[: experts - 1], sem.at[k])

    def update(k):
        if FIRST[k] == "z":
            wait_ring(k)
        else:
            all_of(k, zrecv[k], z_recv).wait()
        for copy in load_states(k):
            copy.wait()

        def step(s, n):
            source = source_s[s]
            arrived = ring_sum(k, x, source) if FIRST[k] == "z" else zrecv[k][source].astype(F32)
            for unit in range(CHUNKS[k]):
                for row in range(2):
                    woven[n, pl.ds(unit * 16 + row, TILES, stride=2), :] = arrived[
                        unit * 16 + row * 8 : unit * 16 + row * 8 + 8
                    ]
            rows = CHUNKS[k] * 16
            (params, first, second) = adam(woven[n, :rows], master_v[k][s], first_v[k][s], second_v[k][s])
            params_out[s, own_rows(k), :] = params
            first_out[s, pl.ds(starts[k] * 16, rows), :] = first
            second_out[s, pl.ds(starts[k] * 16, rows), :] = second

        def some(g, carry):
            for n in range(UNROLL):
                step(g * UNROLL + n, n)
            return carry

        lax.fori_loop(0, blocks // UNROLL, some, 0)

    for n, (stage, number) in enumerate(ORDER):
        k = int(number)
        copies = []
        if stage == "S":
            look_up()
        elif stage == "W":
            weigh(k)
            copies = far_copies(k) if FIRST[k] == "y" else [x_copy(k)]
        elif stage == "D":
            add_x(k)
            if FIRST[k] == "x":
                copies = far_copies(k)
            else:
                to_owners(k)
        elif stage == "E":
            all_of(k, zrecv[k], z_recv).wait()
            copies = far_copies(k)
        elif stage == "P":
            add_on_way(k)
            copies = pass_copies(k)
        elif stage == "L":
            copies = plain_copies(k)
        elif stage == "X" and FIRST[k] == "y":
            x_half(k)
            copies = [x_copy(k)]
        elif stage == "Z":
            finish(k)
            to_owners(k)
        elif stage == "U":
            update(k)
            copies = [t_copy(k)]
        if n == 0:
            pl.semaphore_wait(barrier, experts + 3)
        for copy in copies:
            copy.start()

    for k in range(chunks):
        for copy in far_copies(k) + pass_copies(k) + plain_copies(k) + [x_copy(k)]:
            copy.wait_send()
        all_of(k, zsend[k], z_send).wait()
        t_copy(k).wait()


def fused(experts, blocks, *operands):
    chunks = len(CHUNKS)
    units = sum(CHUNKS)
    wide = max(CHUNKS)

    def each(*lead, dtype=BF16):
        return [pltpu.VMEM((*lead, n * 16, LANES), dtype) for n in CHUNKS]

    scratch = [pltpu.VMEM((blocks, 2, n * 64, LANES), BF16) for n in CHUNKS]
    def by_order(first, then):
        return [
            pltpu.VMEM((*(first if way == "y" else then), n * 16, LANES), BF16) for n, way in zip(CHUNKS, FIRST)
        ]

    scratch += each(2 * RING, experts)
    for _ in range(3):
        scratch += by_order((2, experts), (experts,))
    for _ in range(2):
        scratch += by_order((experts,), (RING, experts))
    for _ in range(2):
        scratch += [
            pltpu.VMEM((experts, *((RING,) if way == "z" else ()), n * 16, LANES), BF16)
            for n, way in zip(CHUNKS, FIRST)
        ]
    scratch += each(blocks, dtype=F32) + each(blocks, dtype=F32) + each(blocks, dtype=F32)
    scratch += [pltpu.VMEM((UNROLL, 2, wide * 64, LANES), F32), pltpu.VMEM((UNROLL, wide * 16, LANES), F32)]
    scratch += [pltpu.VMEM(operands[0].shape, jnp.int32), pltpu.SMEM(operands[1].shape, jnp.int32)]
    scratch += [pltpu.SMEM((experts,), jnp.int32), pltpu.SMEM((blocks,), jnp.int32)]
    scratch += [pltpu.SemaphoreType.DMA((n,)) for n in (2,)]
    scratch += [pltpu.SemaphoreType.DMA((n * chunks,)) for n in (4, 2, 2, 2, 2, 2, 2, 1, 1, 1, 1, 1, 1)]
    return pl.pallas_call(
        lambda *refs: kernel(experts, blocks, refs),
        name="outer_step",
        out_shape=(
            pltpu.VMEM((blocks, 2 * units * 16, LANES), BF16),
            pltpu.VMEM((blocks, units * 16, LANES), F32),
            pltpu.VMEM((blocks, units * 16, LANES), F32),
        ),
        in_specs=[pl.BlockSpec(memory_space=pltpu.HBM)] * len(operands),
        out_specs=(pl.BlockSpec(memory_space=pltpu.VMEM),) * 3,
        scratch_shapes=scratch,
        compiler_params=pltpu.CompilerParams(
            collective_id=0, has_side_effects=True, vmem_limit_bytes=32 * 1024 * 1024
        ),
    )(*(pltpu.with_memory_space_constraint(value, pltpu.HBM) for value in operands))


def store(*refs):
    count = len(refs) // 2
    sem = refs[-1]
    copies = [pltpu.make_async_copy(refs[n], refs[count + n], sem.at[n]) for n in range(count)]
    for copy in copies:
        copy.start()
    for copy in copies:
        copy.wait()


def stored(*values):
    return pl.pallas_call(
        store,
        name="store",
        out_shape=tuple(jax.ShapeDtypeStruct(value.shape, value.dtype) for value in values),
        in_specs=[pl.BlockSpec(memory_space=pltpu.VMEM)] * len(values),
        out_specs=(pl.BlockSpec(memory_space=pltpu.HBM),) * len(values),
        scratch_shapes=[pltpu.SemaphoreType.DMA((len(values),))],
        compiler_params=pltpu.CompilerParams(vmem_limit_bytes=8 * 1024 * 1024),
    )(*values)


def tiled(value, rows):
    lead = value.shape[:-2]
    tall, columns = value.shape[-2:]
    split = value.reshape(*lead, tall // rows, rows, columns // LANES, LANES)
    return jnp.swapaxes(split, -3, -2).reshape(*lead, tall // rows, columns // LANES * rows, LANES)


def untiled(value):
    lead, tall, lanes = value.shape
    split = value.reshape(lead, tall // 2, 2, lanes)
    return jnp.swapaxes(split, 1, 2).reshape(lead, 2, tall // 2 * lanes)


def body(experts, delta, step_offsets, block_map, master_params, first_moment, second_moment):
    blocks = master_params.shape[0]
    states = [tiled(value, 2)[:, 0] for value in (master_params, first_moment, second_moment)]
    outs = fused(experts, blocks, step_offsets[None], block_map, tiled(delta[0], 8), *states)
    return tuple(untiled(value) for value in stored(*outs))


def solution(mesh):
    in_specs = (
        P("replica", "expert", None, "tensor"),
        P(),
        P(),
        P("expert", "replica", "tensor"),
        P("expert", "replica", "tensor"),
        P("expert", "replica", "tensor"),
    )
    out_specs = (
        P("expert", "replica", None),
        P("expert", "replica", "tensor"),
        P("expert", "replica", "tensor"),
    )
    step = functools.partial(body, mesh.shape["expert"])
    return jax.shard_map(step, mesh=mesh, in_specs=in_specs, out_specs=out_specs, check_vma=False)
```

```python
import functools

import jax
import jax.numpy as jnp
from jax import lax
from jax.experimental import pallas as pl
from jax.experimental.pallas import tpu as pltpu
from jax.sharding import PartitionSpec as P

beta_one = 0.9
beta_two = 0.99
outer_rate = 0.7
outer_round = 20
epsilon = 1e-08

MESH = pl.DeviceIdType.MESH
F32 = jnp.float32
BF16 = jnp.bfloat16

CHUNKS = (1, 1, 1, 1, 1, 1, 1)
FIRST = "yyyyxxz"
ORDER = (
    "W6", "W3", "W2", "W0", "L2", "L0", "S0", "W4", "P2", "W1", "L3", "P0", "P3", "D6", "X2", "W5", "D4", "P1", "Z2", "L4", "P4", "L1", "X0", "E6", "X3", "Z4", "D5", "X1", "L5", "Z0", "L6", "P6", "Z3", "P5", "U2", "Z1", "U6", "U4", "Z5", "U0", "U3", "U1", "U5",
)
LANES = 128
TILES = 8
RING = 4
UNROLL = 4


def adam(gradient, master, first, second):
    new_first = beta_one * first + (1.0 - beta_one) * gradient
    new_second = beta_two * second + (1.0 - beta_two) * gradient * gradient
    fix_one = 1.0 - beta_one**outer_round
    fix_two = 1.0 - beta_two**outer_round
    step = new_first / fix_one / (jnp.sqrt(new_second / fix_two) + epsilon)
    return (master - outer_rate * step).astype(BF16), new_first, new_second


def kernel(experts, blocks, refs):
    chunks = len(CHUNKS)
    starts = [sum(CHUNKS[:k]) for k in range(chunks)]
    (offsets_hbm, map_hbm, delta_ref, master_ref, first_ref, second_ref) = refs[:6]
    (params_out, first_out, second_out) = refs[6:9]
    scratch = list(refs[9:])

    def take(n):
        got = scratch[:n]
        del scratch[:n]
        return got

    delta_v = take(chunks)
    weighted = take(chunks)
    far = take(chunks)
    passed = take(chunks)
    plain = take(chunks)
    xsend = take(chunks)
    xrecv = take(chunks)
    zsend = take(chunks)
    zrecv = take(chunks)
    master_v = take(chunks)
    first_v = take(chunks)
    second_v = take(chunks)
    (spread, woven) = take(2)
    (offsets_ref, map_ref, order_s, source_s) = take(4)
    (small_sem, in_sem, far_send, far_recv, pass_send, pass_recv, plain_send, plain_recv) = take(8)
    (x_send, x_recv, z_send, z_recv, t_send, t_recv) = take(6)

    replica = lax.axis_index("replica")
    expert = lax.axis_index("expert")
    tensor = lax.axis_index("tensor")
    x = replica // RING
    y = replica % RING
    up = (y + 1) % RING
    down = (y + RING - 1) % RING
    across = (y + 2) % RING
    device_up = {"replica": x * RING + up}
    device_down = {"replica": x * RING + down}
    device_x = {"replica": (1 - x) * RING + y}
    device_t = {"tensor": 1 - tensor}

    def load_delta(k):
        rows = pl.ds(starts[k] * TILES * 8, CHUNKS[k] * TILES * 8)
        return pltpu.make_async_copy(delta_ref.at[:, :, rows, :], delta_v[k], in_sem.at[k])

    def load_states(k):
        rows = pl.ds(starts[k] * 16, CHUNKS[k] * 16)
        return [
            pltpu.make_async_copy(ref.at[:, rows, :], held[k], in_sem.at[(n + 1) * chunks + k])
            for n, (ref, held) in enumerate(
                ((master_ref, master_v), (first_ref, first_v), (second_ref, second_v))
            )
        ]

    load_map = pltpu.make_async_copy(map_hbm, map_ref, small_sem.at[0])
    load_offsets = pltpu.make_async_copy(offsets_hbm, offsets_ref, small_sem.at[1])
    load_map.start()
    load_offsets.start()
    first_used = [int(number) for stage, number in ORDER if stage == "W"]
    for k in first_used:
        load_delta(k).start()
    for k in range(chunks):
        for copy in load_states(k):
            copy.start()

    barrier = pltpu.get_barrier_semaphore()
    for device in (device_up, device_down, device_x, device_t):
        pl.semaphore_signal(barrier, inc=1, device_id=device, device_id_type=MESH)

    def greet(d, carry):
        pl.semaphore_signal(
            barrier, inc=1, device_id={"expert": (expert + d) % experts}, device_id_type=MESH
        )
        return carry

    lax.fori_loop(1, experts, greet, 0)

    load_offsets.wait()
    reciprocal = 1.0 / (1.0 + offsets_ref[...].astype(F32))
    weights = reciprocal / jnp.sum(reciprocal, axis=1, keepdims=True)
    lane = lax.broadcasted_iota(jnp.int32, weights.shape, 1)
    weight = jnp.sum(jnp.where(lane == replica, weights, 0.0), axis=1, keepdims=True)

    def look_up():
        load_map.wait()

        def find_order(b, held):
            target = lax.shift_right_logical(map_ref[expert * blocks + b], 4)
            return tuple(jnp.where(target == j, b, held[j]) for j in range(experts))

        order = lax.fori_loop(0, blocks, find_order, (jnp.int32(0),) * experts)
        for j in range(experts):
            order_s[j] = order[j]

        def find_source(i, held):
            slot = jnp.int32(0)
            for b in range(blocks):
                owner = map_ref[i * blocks + b]
                slot = jnp.where(lax.shift_right_logical(owner, 4) == expert, owner, slot)
            slot = slot - expert * blocks
            return tuple(jnp.where(slot == s, i, held[s]) for s in range(blocks))

        source = lax.fori_loop(0, experts, find_source, (jnp.int32(0),) * blocks)
        for s in range(blocks):
            source_s[s] = source[s]

    def remote(src, dst, send, recv, device):
        return pltpu.make_async_remote_copy(
            src_ref=src, dst_ref=dst, send_sem=send, recv_sem=recv, device_id=device, device_id_type=MESH
        )

    half = experts // 2
    low, high = pl.ds(0, half), pl.ds(half, half)

    def both_ways(k, up_from, up_to, down_from, down_to, send, recv):
        return [
            remote(up_from, up_to, send.at[2 * k], recv.at[2 * k], device_up),
            remote(down_from, down_to, send.at[2 * k + 1], recv.at[2 * k + 1], device_down),
        ]

    def y_term(k, place, rows):
        return xsend[k].at[place, rows] if FIRST[k] == "x" else zrecv[k].at[rows, place]

    def far_copies(k):
        if FIRST[k] == "y":
            ends = (weighted[k].at[across], far[k].at[0], weighted[k].at[RING + across], far[k].at[1])
        else:
            ends = (y_term(k, across, low), far[k].at[low], y_term(k, across, high), far[k].at[high])
        return both_ways(k, *ends, far_send, far_recv)

    def pass_copies(k):
        if FIRST[k] == "y":
            ends = (far[k].at[0], passed[k].at[0], far[k].at[1], passed[k].at[1])
        else:
            ends = (far[k].at[low], passed[k].at[low], far[k].at[high], passed[k].at[high])
        return both_ways(k, *ends, pass_send, pass_recv)

    def plain_copies(k):
        if FIRST[k] == "y":
            ends = (weighted[k].at[RING + up], plain[k].at[1], weighted[k].at[down], plain[k].at[0])
        else:
            ends = (y_term(k, up, high), plain[k].at[high], y_term(k, down, low), plain[k].at[low])
        return both_ways(k, *ends, plain_send, plain_recv)

    def x_copy(k):
        source = xsend[k] if FIRST[k] == "y" else weighted[k].at[pl.ds(RING * (1 - x), RING)]
        return remote(source, xrecv[k], x_send.at[k], x_recv.at[k], device_x)

    def z_copy(k, j):
        return remote(zsend[k].at[j], zrecv[k].at[expert], z_send.at[k], z_recv.at[k], {"expert": j})

    def own_rows(k):
        whole = CHUNKS[k] * 16
        return pl.ds(pl.multiple_of(tensor * (sum(CHUNKS) * 16) + starts[k] * 16, 16), whole)

    def t_copy(k):
        return remote(params_out.at[:, own_rows(k), :], params_out.at[:, own_rows(k), :], t_send.at[k], t_recv.at[k], device_t)

    def weigh(k):
        units = CHUNKS[k]
        load_delta(k).wait()

        def some(g, carry):
            for n in range(UNROLL):
                j = g * UNROLL + n
                for h in range(2):
                    spread[n, h, : units * 64, :] = delta_v[k][j, h].astype(F32) * weight
                for h in range(2):
                    for q in range(RING):
                        for unit in range(units):
                            pair = [
                                spread[n, h, pl.ds(unit * 64 + 2 * q + row, TILES, stride=8), :] for row in range(2)
                            ]
                            weighted[k][RING * h + q, j, unit * 16 : unit * 16 + 16, :] = jnp.concatenate(
                                pair, axis=0
                            ).astype(BF16)
            return carry

        lax.fori_loop(0, experts // UNROLL, some, 0)

    def loop(step):
        def some(g, carry):
            for n in range(UNROLL):
                step(g * UNROLL + n)
            return carry

        lax.fori_loop(0, experts // UNROLL, some, 0)

    def add_x(k):
        x_copy(k).wait_recv()

        def x_sum(q, j):
            return (weighted[k][RING * x + q, j].astype(F32) + xrecv[k][q, j].astype(F32)).astype(BF16)

        def step(j):
            for q in range(RING):
                if FIRST[k] == "x":
                    xsend[k][q, j] = x_sum(q, j)
                else:
                    zsend[k][j, q] = x_sum(q, order_s[j])

        loop(step)

    def add_on_way(k):
        for copy in far_copies(k):
            copy.wait_recv()

        def step(j):
            for n, place in ((0, up), (1, RING + down)):
                total = far[k][n, j].astype(F32) + weighted[k][place, j].astype(F32)
                far[k][n, j] = total.astype(BF16)

        def step_half(g, carry):
            for n in range(2):
                for base, place in ((0, up), (half, down)):
                    j = base + g * 2 + n
                    own = xsend[k][place, j] if FIRST[k] == "x" else zrecv[k][j, place]
                    far[k][j] = (far[k][j].astype(F32) + own.astype(F32)).astype(BF16)
            return carry

        if FIRST[k] == "y":
            loop(step)
        else:
            lax.fori_loop(0, half // 2, step_half, 0)

    def ring_sum(k, h, j):
        if FIRST[k] == "y":
            terms = (weighted[k][RING * h + y, j], plain[k][h, j], passed[k][h, j])
        elif FIRST[k] == "x":
            terms = (xsend[k][y, j], plain[k][j], passed[k][j])
        else:
            terms = (zrecv[k][j, y], plain[k][j], passed[k][j])
        return terms[0].astype(F32) + terms[1].astype(F32) + terms[2].astype(F32)

    def wait_ring(k):
        for copy in pass_copies(k) + plain_copies(k):
            copy.wait_recv()

    def x_half(k):
        wait_ring(k)

        def step(j):
            xsend[k][j] = ring_sum(k, 1 - x, j).astype(BF16)

        loop(step)

    def finish(k):
        if FIRST[k] == "y":
            x_copy(k).wait_recv()
        else:
            wait_ring(k)

        def step(j):
            block = order_s[j]
            total = ring_sum(k, x, block)
            if FIRST[k] == "y":
                total = total + xrecv[k][block].astype(F32)
            zsend[k][j] = total.astype(BF16)

        loop(step)

    def to_owners(k):
        for i in range(experts - 1):
            turn = i // 2
            hops = (turn + 1) // 2 * (1 - 2 * (turn % 2)) + experts // 4
            z = (expert // 2 + hops) % (experts // 2)
            z_copy(k, 2 * z + (expert + 1 + i) % 2).start()
        zrecv[k][expert] = zsend[k][expert]

    def all_of(k, ref, sem):
        return pltpu.make_async_copy(ref.at[: experts - 1], ref.at[: experts - 1], sem.at[k])

    def update(k):
        if FIRST[k] == "z":
            wait_ring(k)
        else:
            all_of(k, zrecv[k], z_recv).wait()
        for copy in load_states(k):
            copy.wait()

        def step(s, n):
            source = source_s[s]
            arrived = ring_sum(k, x, source) if FIRST[k] == "z" else zrecv[k][source].astype(F32)
            for unit in range(CHUNKS[k]):
                for row in range(2):
                    woven[n, pl.ds(unit * 16 + row, TILES, stride=2), :] = arrived[
                        unit * 16 + row * 8 : unit * 16 + row * 8 + 8
                    ]
            rows = CHUNKS[k] * 16
            (params, first, second) = adam(woven[n, :rows], master_v[k][s], first_v[k][s], second_v[k][s])
            params_out[s, own_rows(k), :] = params
            first_out[s, pl.ds(starts[k] * 16, rows), :] = first
            second_out[s, pl.ds(starts[k] * 16, rows), :] = second

        def some(g, carry):
            for n in range(UNROLL):
                step(g * UNROLL + n, n)
            return carry

        lax.fori_loop(0, blocks // UNROLL, some, 0)

    for n, (stage, number) in enumerate(ORDER):
        k = int(number)
        copies = []
        if stage == "S":
            look_up()
        elif stage == "W":
            weigh(k)
            copies = far_copies(k) if FIRST[k] == "y" else [x_copy(k)]
        elif stage == "D":
            add_x(k)
            if FIRST[k] == "x":
                copies = far_copies(k)
            else:
                to_owners(k)
        elif stage == "E":
            all_of(k, zrecv[k], z_recv).wait()
            copies = far_copies(k)
        elif stage == "P":
            add_on_way(k)
            copies = pass_copies(k)
        elif stage == "L":
            copies = plain_copies(k)
        elif stage == "X" and FIRST[k] == "y":
            x_half(k)
            copies = [x_copy(k)]
        elif stage == "Z":
            finish(k)
            to_owners(k)
        elif stage == "U":
            update(k)
            copies = [t_copy(k)]
        if n == 0:
            pl.semaphore_wait(barrier, experts + 3)
        for copy in copies:
            copy.start()

    for k in range(chunks):
        for copy in far_copies(k) + pass_copies(k) + plain_copies(k) + [x_copy(k)]:
            copy.wait_send()
        all_of(k, zsend[k], z_send).wait()
    for stage, number in ORDER:
        if stage == "U":
            t_copy(int(number)).wait()


def fused(experts, blocks, *operands):
    chunks = len(CHUNKS)
    units = sum(CHUNKS)
    wide = max(CHUNKS)

    def each(*lead, dtype=BF16):
        return [pltpu.VMEM((*lead, n * 16, LANES), dtype) for n in CHUNKS]

    scratch = [pltpu.VMEM((blocks, 2, n * 64, LANES), BF16) for n in CHUNKS]
    def by_order(first, then):
        return [
            pltpu.VMEM((*(first if way == "y" else then), n * 16, LANES), BF16) for n, way in zip(CHUNKS, FIRST)
        ]

    scratch += each(2 * RING, experts)
    for _ in range(3):
        scratch += by_order((2, experts), (experts,))
    for _ in range(2):
        scratch += by_order((experts,), (RING, experts))
    for _ in range(2):
        scratch += [
            pltpu.VMEM((experts, *((RING,) if way == "z" else ()), n * 16, LANES), BF16)
            for n, way in zip(CHUNKS, FIRST)
        ]
    scratch += each(blocks, dtype=F32) + each(blocks, dtype=F32) + each(blocks, dtype=F32)
    scratch += [pltpu.VMEM((UNROLL, 2, wide * 64, LANES), F32), pltpu.VMEM((UNROLL, wide * 16, LANES), F32)]
    scratch += [pltpu.VMEM(operands[0].shape, jnp.int32), pltpu.SMEM(operands[1].shape, jnp.int32)]
    scratch += [pltpu.SMEM((experts,), jnp.int32), pltpu.SMEM((blocks,), jnp.int32)]
    scratch += [pltpu.SemaphoreType.DMA((n,)) for n in (2,)]
    scratch += [pltpu.SemaphoreType.DMA((n * chunks,)) for n in (4, 2, 2, 2, 2, 2, 2, 1, 1, 1, 1, 1, 1)]
    return pl.pallas_call(
        lambda *refs: kernel(experts, blocks, refs),
        name="outer_step",
        out_shape=(
            pltpu.VMEM((blocks, 2 * units * 16, LANES), BF16),
            pltpu.VMEM((blocks, units * 16, LANES), F32),
            pltpu.VMEM((blocks, units * 16, LANES), F32),
        ),
        in_specs=[pl.BlockSpec(memory_space=pltpu.HBM)] * len(operands),
        out_specs=(pl.BlockSpec(memory_space=pltpu.VMEM),) * 3,
        scratch_shapes=scratch,
        compiler_params=pltpu.CompilerParams(
            collective_id=0, has_side_effects=True, vmem_limit_bytes=32 * 1024 * 1024
        ),
    )(*(pltpu.with_memory_space_constraint(value, pltpu.HBM) for value in operands))


def store(*refs):
    count = len(refs) // 2
    sem = refs[-1]
    copies = [pltpu.make_async_copy(refs[n], refs[count + n], sem.at[n]) for n in range(count)]
    for copy in copies:
        copy.start()
    for copy in copies:
        copy.wait()


def stored(*values):
    return pl.pallas_call(
        store,
        name="store",
        out_shape=tuple(jax.ShapeDtypeStruct(value.shape, value.dtype) for value in values),
        in_specs=[pl.BlockSpec(memory_space=pltpu.VMEM)] * len(values),
        out_specs=(pl.BlockSpec(memory_space=pltpu.HBM),) * len(values),
        scratch_shapes=[pltpu.SemaphoreType.DMA((len(values),))],
        compiler_params=pltpu.CompilerParams(vmem_limit_bytes=8 * 1024 * 1024),
    )(*values)


def tiled(value, rows):
    lead = value.shape[:-2]
    tall, columns = value.shape[-2:]
    split = value.reshape(*lead, tall // rows, rows, columns // LANES, LANES)
    return jnp.swapaxes(split, -3, -2).reshape(*lead, tall // rows, columns // LANES * rows, LANES)


def untiled(value):
    lead, tall, lanes = value.shape
    split = value.reshape(lead, tall // 2, 2, lanes)
    return jnp.swapaxes(split, 1, 2).reshape(lead, 2, tall // 2 * lanes)


def body(experts, delta, step_offsets, block_map, master_params, first_moment, second_moment):
    blocks = master_params.shape[0]
    states = [tiled(value, 2)[:, 0] for value in (master_params, first_moment, second_moment)]
    outs = fused(experts, blocks, step_offsets[None], block_map, tiled(delta[0], 8), *states)
    return tuple(untiled(value) for value in stored(*outs))


def solution(mesh):
    in_specs = (
        P("replica", "expert", None, "tensor"),
        P(),
        P(),
        P("expert", "replica", "tensor"),
        P("expert", "replica", "tensor"),
        P("expert", "replica", "tensor"),
    )
    out_specs = (
        P("expert", "replica", None),
        P("expert", "replica", "tensor"),
        P("expert", "replica", "tensor"),
    )
    step = functools.partial(body, mesh.shape["expert"])
    return jax.shard_map(step, mesh=mesh, in_specs=in_specs, out_specs=out_specs, check_vma=False)
```

```python
import functools

import jax
import jax.numpy as jnp
from jax import lax
from jax.experimental import pallas as pl
from jax.experimental.pallas import tpu as pltpu
from jax.sharding import PartitionSpec as P

beta_one = 0.9
beta_two = 0.99
outer_rate = 0.7
outer_round = 20
epsilon = 1e-08

MESH = pl.DeviceIdType.MESH
F32 = jnp.float32
BF16 = jnp.bfloat16

CHUNKS = (1, 1, 1, 1, 1, 1, 1)
FIRST = "yyyyxxz"
ORDER = (
    "W6", "W3", "W2", "W0", "L2", "L0", "S0", "W4", "P2", "W1", "L3", "P0", "P3", "D6", "X2", "W5", "D4", "P1", "Z2", "L4", "P4", "L1", "X0", "E6", "X3", "Z4", "D5", "X1", "L5", "Z0", "L6", "P6", "Z3", "P5", "U2", "Z1", "U6", "U4", "Z5", "U0", "U3", "U1", "U5",
)
LANES = 128
TILES = 8
RING = 4
UNROLL = 8


def adam(gradient, master, first, second):
    new_first = beta_one * first + (1.0 - beta_one) * gradient
    new_second = beta_two * second + (1.0 - beta_two) * gradient * gradient
    fix_one = 1.0 - beta_one**outer_round
    fix_two = 1.0 - beta_two**outer_round
    step = new_first / fix_one / (jnp.sqrt(new_second / fix_two) + epsilon)
    return (master - outer_rate * step).astype(BF16), new_first, new_second


def kernel(experts, blocks, refs):
    chunks = len(CHUNKS)
    starts = [sum(CHUNKS[:k]) for k in range(chunks)]
    (offsets_hbm, map_hbm, delta_ref, master_ref, first_ref, second_ref) = refs[:6]
    (params_out, first_out, second_out) = refs[6:9]
    scratch = list(refs[9:])

    def take(n):
        got = scratch[:n]
        del scratch[:n]
        return got

    delta_v = take(chunks)
    weighted = take(chunks)
    far = take(chunks)
    passed = take(chunks)
    plain = take(chunks)
    xsend = take(chunks)
    xrecv = take(chunks)
    zsend = take(chunks)
    zrecv = take(chunks)
    master_v = take(chunks)
    first_v = take(chunks)
    second_v = take(chunks)
    (spread, woven) = take(2)
    (offsets_ref, map_ref, order_s, source_s) = take(4)
    (small_sem, in_sem, far_send, far_recv, pass_send, pass_recv, plain_send, plain_recv) = take(8)
    (x_send, x_recv, z_send, z_recv, t_send, t_recv) = take(6)

    replica = lax.axis_index("replica")
    expert = lax.axis_index("expert")
    tensor = lax.axis_index("tensor")
    x = replica // RING
    y = replica % RING
    up = (y + 1) % RING
    down = (y + RING - 1) % RING
    across = (y + 2) % RING
    device_up = {"replica": x * RING + up}
    device_down = {"replica": x * RING + down}
    device_x = {"replica": (1 - x) * RING + y}
    device_t = {"tensor": 1 - tensor}

    def load_delta(k):
        rows = pl.ds(starts[k] * TILES * 8, CHUNKS[k] * TILES * 8)
        return pltpu.make_async_copy(delta_ref.at[:, :, rows, :], delta_v[k], in_sem.at[k])

    def load_states(k):
        rows = pl.ds(starts[k] * 16, CHUNKS[k] * 16)
        return [
            pltpu.make_async_copy(ref.at[:, rows, :], held[k], in_sem.at[(n + 1) * chunks + k])
            for n, (ref, held) in enumerate(
                ((master_ref, master_v), (first_ref, first_v), (second_ref, second_v))
            )
        ]

    load_map = pltpu.make_async_copy(map_hbm, map_ref, small_sem.at[0])
    load_offsets = pltpu.make_async_copy(offsets_hbm, offsets_ref, small_sem.at[1])
    load_map.start()
    load_offsets.start()
    first_used = [int(number) for stage, number in ORDER if stage == "W"]
    for k in first_used:
        load_delta(k).start()
    for k in range(chunks):
        for copy in load_states(k):
            copy.start()

    barrier = pltpu.get_barrier_semaphore()
    for device in (device_up, device_down, device_x, device_t):
        pl.semaphore_signal(barrier, inc=1, device_id=device, device_id_type=MESH)

    def greet(d, carry):
        pl.semaphore_signal(
            barrier, inc=1, device_id={"expert": (expert + d) % experts}, device_id_type=MESH
        )
        return carry

    lax.fori_loop(1, experts, greet, 0)

    load_offsets.wait()
    reciprocal = 1.0 / (1.0 + offsets_ref[...].astype(F32))
    weights = reciprocal / jnp.sum(reciprocal, axis=1, keepdims=True)
    lane = lax.broadcasted_iota(jnp.int32, weights.shape, 1)
    weight = jnp.sum(jnp.where(lane == replica, weights, 0.0), axis=1, keepdims=True)

    def look_up():
        load_map.wait()

        def find_order(b, held):
            target = lax.shift_right_logical(map_ref[expert * blocks + b], 4)
            return tuple(jnp.where(target == j, b, held[j]) for j in range(experts))

        order = lax.fori_loop(0, blocks, find_order, (jnp.int32(0),) * experts)
        for j in range(experts):
            order_s[j] = order[j]

        def find_source(i, held):
            slot = jnp.int32(0)
            for b in range(blocks):
                owner = map_ref[i * blocks + b]
                slot = jnp.where(lax.shift_right_logical(owner, 4) == expert, owner, slot)
            slot = slot - expert * blocks
            return tuple(jnp.where(slot == s, i, held[s]) for s in range(blocks))

        source = lax.fori_loop(0, experts, find_source, (jnp.int32(0),) * blocks)
        for s in range(blocks):
            source_s[s] = source[s]

    def remote(src, dst, send, recv, device):
        return pltpu.make_async_remote_copy(
            src_ref=src, dst_ref=dst, send_sem=send, recv_sem=recv, device_id=device, device_id_type=MESH
        )

    half = experts // 2
    low, high = pl.ds(0, half), pl.ds(half, half)

    def both_ways(k, up_from, up_to, down_from, down_to, send, recv):
        return [
            remote(up_from, up_to, send.at[2 * k], recv.at[2 * k], device_up),
            remote(down_from, down_to, send.at[2 * k + 1], recv.at[2 * k + 1], device_down),
        ]

    def y_term(k, place, rows):
        return xsend[k].at[place, rows] if FIRST[k] == "x" else zrecv[k].at[rows, place]

    def far_copies(k):
        if FIRST[k] == "y":
            ends = (weighted[k].at[across], far[k].at[0], weighted[k].at[RING + across], far[k].at[1])
        else:
            ends = (y_term(k, across, low), far[k].at[low], y_term(k, across, high), far[k].at[high])
        return both_ways(k, *ends, far_send, far_recv)

    def pass_copies(k):
        if FIRST[k] == "y":
            ends = (far[k].at[0], passed[k].at[0], far[k].at[1], passed[k].at[1])
        else:
            ends = (far[k].at[low], passed[k].at[low], far[k].at[high], passed[k].at[high])
        return both_ways(k, *ends, pass_send, pass_recv)

    def plain_copies(k):
        if FIRST[k] == "y":
            ends = (weighted[k].at[RING + up], plain[k].at[1], weighted[k].at[down], plain[k].at[0])
        else:
            ends = (y_term(k, up, high), plain[k].at[high], y_term(k, down, low), plain[k].at[low])
        return both_ways(k, *ends, plain_send, plain_recv)

    def x_copy(k):
        source = xsend[k] if FIRST[k] == "y" else weighted[k].at[pl.ds(RING * (1 - x), RING)]
        return remote(source, xrecv[k], x_send.at[k], x_recv.at[k], device_x)

    def z_copy(k, j):
        return remote(zsend[k].at[j], zrecv[k].at[expert], z_send.at[k], z_recv.at[k], {"expert": j})

    def own_rows(k):
        whole = CHUNKS[k] * 16
        return pl.ds(pl.multiple_of(tensor * (sum(CHUNKS) * 16) + starts[k] * 16, 16), whole)

    def t_copy(k):
        return remote(params_out.at[:, own_rows(k), :], params_out.at[:, own_rows(k), :], t_send.at[k], t_recv.at[k], device_t)

    def weigh(k):
        units = CHUNKS[k]
        load_delta(k).wait()

        def some(g, carry):
            for n in range(UNROLL):
                j = g * UNROLL + n
                for h in range(2):
                    spread[n, h, : units * 64, :] = delta_v[k][j, h].astype(F32) * weight
                for h in range(2):
                    for q in range(RING):
                        for unit in range(units):
                            pair = [
                                spread[n, h, pl.ds(unit * 64 + 2 * q + row, TILES, stride=8), :] for row in range(2)
                            ]
                            weighted[k][RING * h + q, j, unit * 16 : unit * 16 + 16, :] = jnp.concatenate(
                                pair, axis=0
                            ).astype(BF16)
            return carry

        lax.fori_loop(0, experts // UNROLL, some, 0)

    def loop(step):
        def some(g, carry):
            for n in range(UNROLL):
                step(g * UNROLL + n)
            return carry

        lax.fori_loop(0, experts // UNROLL, some, 0)

    def add_x(k):
        x_copy(k).wait_recv()

        def x_sum(q, j):
            return (weighted[k][RING * x + q, j].astype(F32) + xrecv[k][q, j].astype(F32)).astype(BF16)

        def step(j):
            for q in range(RING):
                if FIRST[k] == "x":
                    xsend[k][q, j] = x_sum(q, j)
                else:
                    zsend[k][j, q] = x_sum(q, order_s[j])

        loop(step)

    def add_on_way(k):
        for copy in far_copies(k):
            copy.wait_recv()

        def step(j):
            for n, place in ((0, up), (1, RING + down)):
                total = far[k][n, j].astype(F32) + weighted[k][place, j].astype(F32)
                far[k][n, j] = total.astype(BF16)

        def step_half(g, carry):
            for n in range(2):
                for base, place in ((0, up), (half, down)):
                    j = base + g * 2 + n
                    own = xsend[k][place, j] if FIRST[k] == "x" else zrecv[k][j, place]
                    far[k][j] = (far[k][j].astype(F32) + own.astype(F32)).astype(BF16)
            return carry

        if FIRST[k] == "y":
            loop(step)
        else:
            lax.fori_loop(0, half // 2, step_half, 0)

    def ring_sum(k, h, j):
        if FIRST[k] == "y":
            terms = (weighted[k][RING * h + y, j], plain[k][h, j], passed[k][h, j])
        elif FIRST[k] == "x":
            terms = (xsend[k][y, j], plain[k][j], passed[k][j])
        else:
            terms = (zrecv[k][j, y], plain[k][j], passed[k][j])
        return terms[0].astype(F32) + terms[1].astype(F32) + terms[2].astype(F32)

    def wait_ring(k):
        for copy in pass_copies(k) + plain_copies(k):
            copy.wait_recv()

    def x_half(k):
        wait_ring(k)

        def step(j):
            xsend[k][j] = ring_sum(k, 1 - x, j).astype(BF16)

        loop(step)

    def finish(k):
        if FIRST[k] == "y":
            x_copy(k).wait_recv()
        else:
            wait_ring(k)

        def step(j):
            block = order_s[j]
            total = ring_sum(k, x, block)
            if FIRST[k] == "y":
                total = total + xrecv[k][block].astype(F32)
            zsend[k][j] = total.astype(BF16)

        loop(step)

    def to_owners(k):
        for i in range(experts - 1):
            turn = i // 2
            hops = (turn + 1) // 2 * (1 - 2 * (turn % 2)) + experts // 4
            z = (expert // 2 + hops) % (experts // 2)
            z_copy(k, 2 * z + (expert + 1 + i) % 2).start()
        zrecv[k][expert] = zsend[k][expert]

    def all_of(k, ref, sem):
        return pltpu.make_async_copy(ref.at[: experts - 1], ref.at[: experts - 1], sem.at[k])

    def update(k):
        if FIRST[k] == "z":
            wait_ring(k)
        else:
            all_of(k, zrecv[k], z_recv).wait()
        for copy in load_states(k):
            copy.wait()

        def step(s, n):
            source = source_s[s]
            arrived = ring_sum(k, x, source) if FIRST[k] == "z" else zrecv[k][source].astype(F32)
            for unit in range(CHUNKS[k]):
                for row in range(2):
                    woven[n, pl.ds(unit * 16 + row, TILES, stride=2), :] = arrived[
                        unit * 16 + row * 8 : unit * 16 + row * 8 + 8
                    ]
            rows = CHUNKS[k] * 16
            (params, first, second) = adam(woven[n, :rows], master_v[k][s], first_v[k][s], second_v[k][s])
            params_out[s, own_rows(k), :] = params
            first_out[s, pl.ds(starts[k] * 16, rows), :] = first
            second_out[s, pl.ds(starts[k] * 16, rows), :] = second

        def some(g, carry):
            for n in range(UNROLL):
                step(g * UNROLL + n, n)
            return carry

        lax.fori_loop(0, blocks // UNROLL, some, 0)

    for n, (stage, number) in enumerate(ORDER):
        k = int(number)
        copies = []
        if stage == "S":
            look_up()
        elif stage == "W":
            weigh(k)
            copies = far_copies(k) if FIRST[k] == "y" else [x_copy(k)]
        elif stage == "D":
            add_x(k)
            if FIRST[k] == "x":
                copies = far_copies(k)
            else:
                to_owners(k)
        elif stage == "E":
            all_of(k, zrecv[k], z_recv).wait()
            copies = far_copies(k)
        elif stage == "P":
            add_on_way(k)
            copies = pass_copies(k)
        elif stage == "L":
            copies = plain_copies(k)
        elif stage == "X" and FIRST[k] == "y":
            x_half(k)
            copies = [x_copy(k)]
        elif stage == "Z":
            finish(k)
            to_owners(k)
        elif stage == "U":
            update(k)
            copies = [t_copy(k)]
        if n == 0:
            pl.semaphore_wait(barrier, experts + 3)
        for copy in copies:
            copy.start()

    for k in range(chunks):
        for copy in far_copies(k) + pass_copies(k) + plain_copies(k) + [x_copy(k)]:
            copy.wait_send()
        all_of(k, zsend[k], z_send).wait()
    for stage, number in ORDER:
        if stage == "U":
            t_copy(int(number)).wait()


def fused(experts, blocks, *operands):
    chunks = len(CHUNKS)
    units = sum(CHUNKS)
    wide = max(CHUNKS)

    def each(*lead, dtype=BF16):
        return [pltpu.VMEM((*lead, n * 16, LANES), dtype) for n in CHUNKS]

    scratch = [pltpu.VMEM((blocks, 2, n * 64, LANES), BF16) for n in CHUNKS]
    def by_order(first, then):
        return [
            pltpu.VMEM((*(first if way == "y" else then), n * 16, LANES), BF16) for n, way in zip(CHUNKS, FIRST)
        ]

    scratch += each(2 * RING, experts)
    for _ in range(3):
        scratch += by_order((2, experts), (experts,))
    for _ in range(2):
        scratch += by_order((experts,), (RING, experts))
    for _ in range(2):
        scratch += [
            pltpu.VMEM((experts, *((RING,) if way == "z" else ()), n * 16, LANES), BF16)
            for n, way in zip(CHUNKS, FIRST)
        ]
    scratch += each(blocks, dtype=F32) + each(blocks, dtype=F32) + each(blocks, dtype=F32)
    scratch += [pltpu.VMEM((UNROLL, 2, wide * 64, LANES), F32), pltpu.VMEM((UNROLL, wide * 16, LANES), F32)]
    scratch += [pltpu.VMEM(operands[0].shape, jnp.int32), pltpu.SMEM(operands[1].shape, jnp.int32)]
    scratch += [pltpu.SMEM((experts,), jnp.int32), pltpu.SMEM((blocks,), jnp.int32)]
    scratch += [pltpu.SemaphoreType.DMA((n,)) for n in (2,)]
    scratch += [pltpu.SemaphoreType.DMA((n * chunks,)) for n in (4, 2, 2, 2, 2, 2, 2, 1, 1, 1, 1, 1, 1)]
    return pl.pallas_call(
        lambda *refs: kernel(experts, blocks, refs),
        name="outer_step",
        out_shape=(
            pltpu.VMEM((blocks, 2 * units * 16, LANES), BF16),
            pltpu.VMEM((blocks, units * 16, LANES), F32),
            pltpu.VMEM((blocks, units * 16, LANES), F32),
        ),
        in_specs=[pl.BlockSpec(memory_space=pltpu.HBM)] * len(operands),
        out_specs=(pl.BlockSpec(memory_space=pltpu.VMEM),) * 3,
        scratch_shapes=scratch,
        compiler_params=pltpu.CompilerParams(
            collective_id=0, has_side_effects=True, vmem_limit_bytes=32 * 1024 * 1024
        ),
    )(*(pltpu.with_memory_space_constraint(value, pltpu.HBM) for value in operands))


def store(*refs):
    count = len(refs) // 2
    sem = refs[-1]
    copies = []
    for n in range(count):
        part = refs[n].shape[0] // 4
        for i in range(4):
            rows = pl.ds(i * part, part)
            copies.append(pltpu.make_async_copy(refs[n].at[rows], refs[count + n].at[rows], sem.at[4 * n + i]))
    for copy in copies:
        copy.start()
    for copy in copies:
        copy.wait()


def stored(*values):
    return pl.pallas_call(
        store,
        name="store",
        out_shape=tuple(jax.ShapeDtypeStruct(value.shape, value.dtype) for value in values),
        in_specs=[pl.BlockSpec(memory_space=pltpu.VMEM)] * len(values),
        out_specs=(pl.BlockSpec(memory_space=pltpu.HBM),) * len(values),
        scratch_shapes=[pltpu.SemaphoreType.DMA((4 * len(values),))],
        compiler_params=pltpu.CompilerParams(vmem_limit_bytes=8 * 1024 * 1024),
    )(*values)


def tiled(value, rows):
    lead = value.shape[:-2]
    tall, columns = value.shape[-2:]
    split = value.reshape(*lead, tall // rows, rows, columns // LANES, LANES)
    return jnp.swapaxes(split, -3, -2).reshape(*lead, tall // rows, columns // LANES * rows, LANES)


def untiled(value):
    lead, tall, lanes = value.shape
    split = value.reshape(lead, tall // 2, 2, lanes)
    return jnp.swapaxes(split, 1, 2).reshape(lead, 2, tall // 2 * lanes)


def body(experts, delta, step_offsets, block_map, master_params, first_moment, second_moment):
    blocks = master_params.shape[0]
    states = [tiled(value, 2)[:, 0] for value in (master_params, first_moment, second_moment)]
    outs = fused(experts, blocks, step_offsets[None], block_map, tiled(delta[0], 8), *states)
    return tuple(untiled(value) for value in stored(*outs))


def solution(mesh):
    in_specs = (
        P("replica", "expert", None, "tensor"),
        P(),
        P(),
        P("expert", "replica", "tensor"),
        P("expert", "replica", "tensor"),
        P("expert", "replica", "tensor"),
    )
    out_specs = (
        P("expert", "replica", None),
        P("expert", "replica", "tensor"),
        P("expert", "replica", "tensor"),
    )
    step = functools.partial(body, mesh.shape["expert"])
    return jax.shard_map(step, mesh=mesh, in_specs=in_specs, out_specs=out_specs, check_vma=False)
```
